256 devices in a mesh: fsdp: 32 (over x_lo, z, core), dp: 8 (over y, x_hi).
Axes of the slice: x: 4 (x_hi: 2, x_lo: 2; x = x_hi * 2 + x_lo), y: 4, z: 8, core: 2. Of those that a mesh axis runs over, the one named last changes fastest.
Arguments:
- inputs: bfloat16 [49152, 4096], P(('fsdp', 'dp')), may hold values from -6 to 6
- grad_out: bfloat16 [49152, 14336], P(('fsdp', 'dp')), may hold values from -0.0068359375 to 0.0068359375
- projection: bfloat16 [4096, 128], P('fsdp'), may hold values from -0.375 to 0.375
- moment: float32 [14336, 128], P('fsdp'), may hold values from -1.5 to 1.5
- second: float32 [14336, 128], P('fsdp'), may hold values from 0.0001 to 0.001
Outputs:
- update: bfloat16 [4096, 14336], P('fsdp')
- new_moment: float32 [14336, 128], P('fsdp')
- new_second: float32 [14336, 128], P('fsdp')
The draws below stay inside these ranges and needn't reach their ends.
All inputs are finite; a program needn't handle non-finite values.
Results may differ from the reference program's by a relative error of at most 0.0051.
Values may be sent and summed in bfloat16 or wider, within the bound.
A program may use at most 64 MiB of HBM per device.

```python
import math
import jax
import jax.numpy as jnp
from jax import lax

D = 4096
FF = 14336
RANK = 128
STEP = 10
TOKENS = 49152


def strengthened(values, rng, source, target, blocks, factor):
    owner, partner = [(jnp.arange(values.shape[position]) // (values.shape[position] // blocks)).reshape([-1 if axis == position else 1 for axis in range(values.ndim)]) for position in (source, target)]
    chosen = jax.random.permutation(rng, blocks)[partner]
    strong = (owner == chosen) | (owner == (partner + blocks // 2) % blocks)
    return jnp.where(strong, factor * values, values)


def block_scale(stream_key, dims, shards, smallest, top_value):
    def one(position, parts):
        draws = jax.random.uniform(jax.random.fold_in(jax.random.fold_in(stream_key, 6), position), (parts,), jnp.float32, smallest / len(shards), top_value / len(shards))
        return jnp.repeat(jnp.exp(draws), dims[position] // parts).reshape((-1,) + (1,) * (len(dims) - position - 1))

    gain = one(*shards[0])
    for cut in shards[1:]:
        gain = gain * one(*cut)
    return gain


def scatter_about(rng, shape, width, reach, cuts=(), held_as=jnp.bfloat16):
    result = jax.random.normal(rng, shape, jnp.float32) * width
    if len(cuts) > 0:
        result = block_scale(rng, shape, cuts, -0.22, 0.18) * result
    return jnp.clip(result, min=-reach, max=reach).astype(held_as)


def gaussian_with(stream_key, shape, spread, bound, split, heavy, dtype=jnp.bfloat16):
    entries = spread * jax.random.normal(stream_key, shape, jnp.float32)
    if split:
        entries = entries * block_scale(stream_key, shape, split, -0.22, 0.18)
    return jnp.clip(strengthened(entries, jax.random.fold_in(stream_key, 3), *heavy), -bound, bound).astype(dtype)


def setup_inputs(seed: int = 0) -> dict:
    splits = jax.random.split(jax.random.key(seed), 6)
    inputs = scatter_about(splits[0], (TOKENS, D), 1.0, 6.0, ((0, 256),))
    grad_out = gaussian_with(splits[1], (TOKENS, FF), (TOKENS * 256) ** -0.5, 0.0068359375, ((0, 256),), (0, 1, 256, 6.0))
    projection = scatter_about(splits[2], (D, RANK), (D // 16) ** -0.5, 0.375, ((0, 32),))
    moment = scatter_about(splits[3], (FF, RANK), 0.25, 1.5, ((0, 32),), jnp.float32)
    second = jnp.clip(jnp.exp(math.log(0.001) - 2.3025852 * jax.random.uniform(splits[4], (FF, RANK), jnp.float32) ** block_scale(splits[4], (FF, RANK), ((0, 32),), -0.2, 0.2)), 0.0001, 0.001)
    return {"inputs": inputs, "grad_out": grad_out, "projection": projection, "moment": moment, "second": second}


def reference(inputs, grad_out, projection, moment, second):
    projected = jnp.dot(inputs, projection, preferred_element_type=jnp.float32).astype(jnp.bfloat16)
    low_rank = lax.dot_general(grad_out, projected, (((0,), (0,)), ((), ())), preferred_element_type=jnp.float32)
    new_moment = 0.9 * moment + 0.1 * low_rank
    new_second = 0.999 * second + 0.001 * (low_rank * low_rank)
    first_fix = 1.0 - 0.9 ** STEP
    second_fix = 1.0 - 0.999 ** STEP
    normalized = (new_moment / first_fix / (jnp.sqrt(new_second / second_fix) + 1e-08)).astype(jnp.bfloat16)
    update = lax.dot_general(projection, normalized, (((1,), (1,)), ((), ())), preferred_element_type=jnp.float32).astype(jnp.bfloat16)
    return (update, new_moment, new_second)
```

```python
import jax
import jax.numpy as jnp
from jax import lax
from jax.experimental import pallas as pl
from jax.experimental.pallas import tpu as pltpu
from jax.sharding import Mesh
from jax.sharding import PartitionSpec as P

STEP = 10
AXES = ("xl", "z", "c", "y", "xh")
FSDP = ("xl", "z", "c")
MESH = pl.DeviceIdType.MESH
F32 = jnp.float32
BF16 = jnp.bfloat16


def adam(low_rank, moment, second):
    new_moment = 0.9 * moment + 0.1 * low_rank
    new_second = 0.999 * second + 0.001 * (low_rank * low_rank)
    return new_moment, new_second


def normalize(new_moment, new_second):
    first_fix = 1.0 - 0.9**STEP
    second_fix = 1.0 - 0.999**STEP
    return (new_moment / first_fix / (jnp.sqrt(new_second / second_fix) + 1e-08)).astype(BF16)


def comm_kernel(
    inputs, grad, proj, moment, second,
    full, lr_out,
    xk, pb, gb, part, pt, ms, t, fwd, own, fsum, u, fwd2, own2, fsum2, w, zr, lr_mine,
    sem_l, sem_x, sem_ps, sem_pr, sem_ts, sem_tr, sem_gs, sem_gr, sem_ms, sem_mr,
    sem_1s, sem_1r, sem_2s, sem_2r, sem_zs, sem_zr, sem_ls, sem_lr,
    sem_gzs, sem_gzr, sem_bs, sem_br, sem_as, sem_ar, sem_ds, sem_dr,
):
    xl, z, c, y, xh = (lax.axis_index(n) for n in AXES)
    x = 2 * xh + xl
    tok = inputs.shape[0]
    rank = proj.shape[1]
    piece = w.shape[2]
    half_cols = gb.shape[2]
    blk = 8 * piece
    other = 1 - c
    pa = x + c * (y - x)
    pb_ = y + c * (x - y)

    def at(xx, yy):
        return {"xl": lax.rem(xx, 2), "xh": lax.div(xx, 2), "y": yy}

    def a_dev(s):
        return at(lax.rem(x + s * (1 - c) + 4, 4), lax.rem(y + s * c + 4, 4))

    def b_dev(s):
        return at(lax.rem(x + s * c + 4, 4), lax.rem(y + s * (1 - c) + 4, 4))

    partner = {"c": other}
    mine_z = lax.div(z, 4) == c

    def remote(src, dst, ssem, rsem, dev):
        return pltpu.make_async_remote_copy(
            src_ref=src, dst_ref=dst, send_sem=ssem, recv_sem=rsem, device_id=dev, device_id_type=MESH
        )

    def cols(i, n):
        return pl.ds(pl.multiple_of(i, 128), n)

    def rows(i, n):
        return pl.ds(pl.multiple_of(i, 16), n)

    p_row = rows((xl * 8 + z) * rank, rank)
    p_load = pltpu.make_async_copy(proj, pb.at[p_row], sem_l.at[0])
    p_load.start()
    mine = rows(c * tok, tok)
    for j in range(16):
        pltpu.make_async_copy(
            inputs.at[:, cols((2 * j + c) * rank, rank)], xk.at[mine, pl.ds(j * rank, rank)], sem_l.at[1]
        ).start()
    for k in range(2):
        pltpu.make_async_copy(
            grad.at[:, cols(k * 2 * half_cols + c * half_cols, half_cols)], gb.at[k, mine], sem_l.at[2 + k]
        ).start()
    m_row = pl.ds(pl.multiple_of(y * piece, 8), piece)
    own_state = jnp.logical_and(mine_z, xh == c)
    gets_state = jnp.logical_and(mine_z, xh != c)
    gives_state = jnp.logical_and(jnp.logical_not(mine_z), xh == c)

    @pl.when(own_state)
    def _():
        pltpu.make_async_copy(moment.at[m_row], ms.at[0], sem_l.at[4]).start()
        pltpu.make_async_copy(second.at[m_row], ms.at[1], sem_l.at[5]).start()

    barrier = pltpu.get_barrier_semaphore()

    def greet(dev):
        pl.semaphore_signal(barrier, inc=1, device_id=dev, device_id_type=MESH)

    for d in range(1, 8):
        greet({"z": lax.rem(z + d, 8)})
    for s in (1, -1):
        greet(at(lax.rem(x + s + 4, 4), y))
    for dx in range(2):
        for dy in range(4):
            for dc in range(2):
                if dx or dy or dc:
                    greet({"xh": lax.rem(xh + dx, 2), "y": lax.rem(y + dy, 4), "c": lax.rem(c + dc, 2)})
    pl.semaphore_wait(barrier, 24)

    p_load.wait()
    sends = []
    for d in (4, 3, 5, 2, 6, 1, 7):
        cp = remote(pb.at[p_row], pb.at[p_row], sem_ps.at[d], sem_pr.at[d], {"z": lax.rem(z + d, 8)})
        cp.start()
        sends.append(cp)
    x_right = at(lax.rem(x + 1, 4), y)
    x_left = at(lax.rem(x + 3, 4), y)

    def forward(rel):
        row = rows((xl * 8 + lax.rem(z + rel, 8)) * rank, rank)
        cp = remote(pb.at[row], pb.at[row], sem_ps.at[8 + rel], sem_pr.at[8 + rel], x_right if rel < 4 else x_left)
        cp.start()
        sends.append(cp)

    forward(0)
    theirs = rows(other * tok, tok)
    for j in range(16):
        remote(
            inputs.at[:, cols((2 * j + other) * rank, rank)], xk.at[mine, pl.ds(j * rank, rank)],
            sem_x.at[0], sem_x.at[1], partner,
        ).start()
    x_swap = remote(xk.at[mine], xk.at[theirs], sem_x.at[0], sem_x.at[1], partner)
    for k in range(2):
        cp = remote(
            grad.at[:, cols(k * 2 * half_cols + other * half_cols, half_cols)], gb.at[k, mine],
            sem_gs.at[k], sem_gr.at[k], partner,
        )
        cp.start()
        sends.append(cp)

    @pl.when(gives_state)
    def _():
        remote(moment.at[m_row], ms.at[0], sem_ms.at[0], sem_mr.at[0], partner).start()
        remote(second.at[m_row], ms.at[1], sem_ms.at[1], sem_mr.at[1], partner).start()

    for d in (1, 7, 2, 6, 3, 5, 4):
        row = rows((xl * 8 + lax.rem(z + 8 - d, 8)) * rank, rank)
        remote(pb.at[row], pb.at[row], sem_ps.at[d], sem_pr.at[d], x_right).wait_recv()
        forward(8 - d)
    for rel in range(8):
        row = rows(((1 - xl) * 8 + lax.rem(z + rel, 8)) * rank, rank)
        remote(pb.at[row], pb.at[row], sem_ps.at[8 + rel], sem_pr.at[8 + rel], x_right).wait_recv()

    pltpu.make_async_copy(xk.at[mine], xk.at[mine], sem_l.at[1]).wait()
    x_swap.wait()
    part[0] = jnp.dot(xk[...], pb[...], preferred_element_type=F32)
    p_swap = remote(part.at[0], part.at[1], sem_ts.at[0], sem_tr.at[0], partner)
    p_swap.start()
    p_swap.wait()
    pt[...] = (part[0] + part[1]).T.astype(BF16)

    for k in range(2):
        pltpu.make_async_copy(gb.at[k, mine], gb.at[k, mine], sem_l.at[2 + k]).wait()
        remote(gb.at[k, theirs], gb.at[k, theirs], sem_gs.at[k], sem_gr.at[k], partner).wait_recv()
    right, left, opp = lax.rem(pa + 1, 4), lax.rem(pa + 3, 4), lax.rem(pa + 2, 4)
    dev_r, dev_l = a_dev(1), a_dev(-1)

    def compute_half(h):
        def body(i, carry):
            zl, k = lax.div(i, 2), lax.rem(i, 2)
            g = gb[k, :, cols((2 * h + zl) * blk, blk)]
            out = lax.dot_general(pt[...], g, (((1,), (0,)), ((), ())), preferred_element_type=F32)
            out = out.T.astype(BF16)
            for s in range(8):
                xx, yy = 2 * (s // 4) + k, s % 4
                t[xx + c * (yy - xx), h, yy + c * (xx - yy), zl] = out[s * piece : (s + 1) * piece]
            return carry

        lax.fori_loop(0, 4, body, 0)

    def go(cp):
        cp.start()
        sends.append(cp)

    compute_half(0)
    go(remote(t.at[opp, 0], fwd.at[0], sem_1s.at[0], sem_1r.at[0], dev_r))
    go(remote(t.at[left, 0], own.at[1, 0], sem_1s.at[3], sem_1r.at[3], dev_l))
    compute_half(1)
    go(remote(t.at[opp, 1], fwd.at[1], sem_1s.at[1], sem_1r.at[1], dev_l))
    go(remote(t.at[right, 1], own.at[0, 1], sem_1s.at[2], sem_1r.at[2], dev_r))

    def arrived(dst, ssem, rsem):
        remote(dst, dst, ssem, rsem, partner).wait_recv()

    def add_loop(n, body):
        def step(i, carry):
            body(i)
            return carry

        lax.fori_loop(0, n, step, 0)

    arrived(fwd.at[0], sem_1s.at[0], sem_1r.at[0])

    def add_f0(i):
        b, zl = lax.div(i, 2), lax.rem(i, 2)
        fsum[0, b, zl] = (fwd[0, b, zl].astype(F32) + t[right, 0, b, zl].astype(F32)).astype(BF16)

    add_loop(8, add_f0)
    go(remote(fsum.at[0], own.at[0, 0], sem_1s.at[4], sem_1r.at[4], dev_r))
    arrived(fwd.at[1], sem_1s.at[1], sem_1r.at[1])

    def add_f1(i):
        b, zl = lax.div(i, 2), lax.rem(i, 2)
        fsum[1, b, zl] = (fwd[1, b, zl].astype(F32) + t[left, 1, b, zl].astype(F32)).astype(BF16)

    add_loop(8, add_f1)
    go(remote(fsum.at[1], own.at[1, 1], sem_1s.at[5], sem_1r.at[5], dev_l))

    right2, left2, opp2 = lax.rem(pb_ + 1, 4), lax.rem(pb_ + 3, 4), lax.rem(pb_ + 2, 4)
    dev_r2, dev_l2 = b_dev(1), b_dev(-1)
    arrived(own.at[1, 0], sem_1s.at[3], sem_1r.at[3])
    arrived(own.at[0, 1], sem_1s.at[2], sem_1r.at[2])

    def sum_half(h):
        def body(i):
            b, zl = lax.div(i, 2), lax.rem(i, 2)
            u[h, b, zl] = (
                own[0, h, b, zl].astype(F32) + own[1, h, b, zl].astype(F32) + t[pa, h, b, zl].astype(F32)
            ).astype(BF16)

        add_loop(8, body)

    arrived(own.at[0, 0], sem_1s.at[4], sem_1r.at[4])
    sum_half(0)
    go(remote(u.at[0, opp2], fwd2.at[0], sem_2s.at[0], sem_2r.at[0], dev_r2))
    go(remote(u.at[0, left2], own2.at[1, 0], sem_2s.at[3], sem_2r.at[3], dev_l2))
    arrived(own.at[1, 1], sem_1s.at[5], sem_1r.at[5])
    sum_half(1)
    go(remote(u.at[1, opp2], fwd2.at[1], sem_2s.at[1], sem_2r.at[1], dev_l2))
    go(remote(u.at[1, right2], own2.at[0, 1], sem_2s.at[2], sem_2r.at[2], dev_r2))
    arrived(fwd2.at[0], sem_2s.at[0], sem_2r.at[0])
    fsum2[0] = (fwd2[0].astype(F32) + u[0, right2].astype(F32)).astype(BF16)
    go(remote(fsum2.at[0], own2.at[0, 0], sem_2s.at[4], sem_2r.at[4], dev_r2))
    arrived(fwd2.at[1], sem_2s.at[1], sem_2r.at[1])
    fsum2[1] = (fwd2[1].astype(F32) + u[1, left2].astype(F32)).astype(BF16)
    go(remote(fsum2.at[1], own2.at[1, 1], sem_2s.at[5], sem_2r.at[5], dev_l2))
    arrived(own2.at[1, 0], sem_2s.at[3], sem_2r.at[3])
    arrived(own2.at[0, 1], sem_2s.at[2], sem_2r.at[2])
    arrived(own2.at[0, 0], sem_2s.at[4], sem_2r.at[4])
    w[0] = (own2[0, 0].astype(F32) + own2[1, 0].astype(F32) + u[0, pb_].astype(F32)).astype(BF16)
    arrived(own2.at[1, 1], sem_2s.at[5], sem_2r.at[5])
    w[1] = (own2[0, 1].astype(F32) + own2[1, 1].astype(F32) + u[1, pb_].astype(F32)).astype(BF16)

    for q in range(4):
        dest = 4 * c + q
        src = w.at[q // 2, q % 2]

        @pl.when(z != dest)
        def _():
            remote(src, zr.at[z], sem_zs.at[q], sem_zr.at[z], {"z": dest}).start()

    nz = z - 4 * c
    hz, lz = lax.rem(lax.div(nz + 8, 2), 2), lax.rem(nz + 8, 2)
    quarter = xh

    @pl.when(mine_z)
    def _():
        total = w[hz, lz].astype(F32)
        for d in range(1, 8):
            src_z = lax.rem(z + d, 8)
            arrived(zr.at[src_z], sem_zs.at[0], sem_zr.at[src_z])
            total = total + zr[src_z].astype(F32)
        lr_mine[...] = total

        @pl.when(own_state)
        def _():
            pltpu.make_async_copy(moment.at[m_row], ms.at[0], sem_l.at[4]).wait()
            pltpu.make_async_copy(second.at[m_row], ms.at[1], sem_l.at[5]).wait()

        @pl.when(gets_state)
        def _():
            arrived(ms.at[0], sem_ms.at[0], sem_mr.at[0])
            arrived(ms.at[1], sem_ms.at[1], sem_mr.at[1])

        new_moment, new_second = adam(total, ms[0], ms[1])
        full[c, pa, hz, pb_, lz] = normalize(new_moment, new_second)
        here = full.at[c, pa, hz, pb_, lz]
        for d in range(1, 8):
            remote(here, here, sem_gzs.at[d], sem_gzr.at[nz], {"z": lax.rem(z + d, 8)}).start()

        for dx in range(2):
            for dy in range(4):
                n = dx * 4 + dy
                dev = {"xh": lax.rem(xh + dx, 2), "y": lax.rem(y + dy, 4), "c": quarter}
                cp = remote(lr_mine, lr_out.at[y], sem_ls.at[n], sem_lr.at[y], dev)
                if n == 0:
                    @pl.when(quarter == c)
                    def _():
                        lr_out[y] = total

                    @pl.when(quarter != c)
                    def _():
                        cp.start()
                else:
                    cp.start()

    for q in range(4):
        @pl.when(z != 4 * c + q)
        def _():
            arrived(full.at[c, pa, q // 2, pb_, q % 2], sem_gzs.at[0], sem_gzr.at[q])

    def chunk2(h, b):
        return full.at[c, pa, h, b]

    def hop(ref, ss, rs, i, dev):
        go(remote(ref, ref, ss.at[i], rs.at[i], dev))

    hop(chunk2(0, pb_), sem_bs, sem_br, 0, dev_r2)
    hop(chunk2(1, pb_), sem_bs, sem_br, 1, dev_l2)
    hop(chunk2(1, pb_), sem_bs, sem_br, 2, dev_r2)
    hop(chunk2(0, pb_), sem_bs, sem_br, 3, dev_l2)
    arrived(chunk2(0, left2), sem_bs.at[0], sem_br.at[0])
    hop(chunk2(0, left2), sem_bs, sem_br, 4, dev_r2)
    arrived(chunk2(1, right2), sem_bs.at[1], sem_br.at[1])
    hop(chunk2(1, right2), sem_bs, sem_br, 5, dev_l2)
    arrived(chunk2(1, left2), sem_bs.at[2], sem_br.at[2])
    arrived(chunk2(0, right2), sem_bs.at[3], sem_br.at[3])

    def chunk(h, a):
        return full.at[c, a, h]

    def pass_on(h, a, i):
        go(remote(chunk(h, a), chunk(h, a), sem_ds.at[i], sem_dr.at[i], partner))

    arrived(chunk2(0, opp2), sem_bs.at[4], sem_br.at[4])
    hop(chunk(0, pa), sem_as, sem_ar, 0, dev_r)
    arrived(chunk2(1, opp2), sem_bs.at[5], sem_br.at[5])
    hop(chunk(1, pa), sem_as, sem_ar, 1, dev_l)
    hop(chunk(1, pa), sem_as, sem_ar, 2, dev_r)
    hop(chunk(0, pa), sem_as, sem_ar, 3, dev_l)
    pass_on(0, pa, 0)
    pass_on(1, pa, 1)
    arrived(chunk(0, left), sem_as.at[0], sem_ar.at[0])
    hop(chunk(0, left), sem_as, sem_ar, 4, dev_r)
    pass_on(0, left, 2)
    arrived(chunk(1, right), sem_as.at[1], sem_ar.at[1])
    hop(chunk(1, right), sem_as, sem_ar, 5, dev_l)
    pass_on(1, right, 3)
    arrived(chunk(1, left), sem_as.at[2], sem_ar.at[2])
    pass_on(1, left, 4)
    arrived(chunk(0, right), sem_as.at[3], sem_ar.at[3])
    pass_on(0, right, 5)
    arrived(chunk(0, opp), sem_as.at[4], sem_ar.at[4])
    pass_on(0, opp, 6)
    arrived(chunk(1, opp), sem_as.at[5], sem_ar.at[5])
    pass_on(1, opp, 7)

    for i in range(8):
        arrived(full.at[other, 0, 0], sem_ds.at[i], sem_dr.at[i])
    src_here = lax.div(z, 4) == c
    for q in range(4):
        local = jnp.logical_and(src_here, jnp.logical_and(xh == c, y == q))

        @pl.when(jnp.logical_not(local))
        def _():
            arrived(lr_out.at[q], sem_ls.at[0], sem_lr.at[q])

    for cp in sends:
        cp.wait_send()

    @pl.when(gives_state)
    def _():
        remote(moment.at[m_row], ms.at[0], sem_ms.at[0], sem_mr.at[0], partner).wait_send()
        remote(second.at[m_row], ms.at[1], sem_ms.at[1], sem_mr.at[1], partner).wait_send()

    for q in range(4):
        @pl.when(z != 4 * c + q)
        def _():
            remote(w.at[q // 2, q % 2], zr.at[z], sem_zs.at[q], sem_zr.at[0], partner).wait_send()

    @pl.when(mine_z)
    def _():
        here = full.at[c, pa, hz, pb_, lz]
        for d in range(1, 8):
            remote(here, here, sem_gzs.at[d], sem_gzr.at[0], partner).wait_send()
        for n in range(8):
            cp = remote(lr_mine, lr_out.at[y], sem_ls.at[n], sem_lr.at[0], partner)
            if n == 0:
                @pl.when(quarter != c)
                def _():
                    cp.wait_send()
            else:
                cp.wait_send()


def update_kernel(full, lr, proj, moment, second, update, new_moment, new_second):
    i = pl.program_id(0)
    xl, z = lax.div(i, 8), lax.rem(i, 8)
    c, h, zl = lax.div(z, 4), lax.div(lax.rem(z, 4), 2), lax.rem(z, 2)
    parts = []
    for s in range(8):
        x, y = 2 * (s // 4) + xl, s % 4
        parts.append(full[c, x + c * (y - x), h, y + c * (x - y), zl])
    block = jnp.concatenate(parts, axis=0)
    update[...] = lax.dot_general(
        proj[...], block, (((1,), (1,)), ((), ())), preferred_element_type=F32
    ).astype(BF16)

    @pl.when(i == 0)
    def _():
        m, s = adam(lr[...], moment[...], second[...])
        new_moment[...] = m
        new_second[...] = s


def local(inputs, grad_out, projection, moment, second):
    tok, ff = grad_out.shape
    rank = projection.shape[1]
    piece = ff // 128
    half = (4, 2, piece, rank)
    small = (2, piece, rank)
    anyspace = pl.BlockSpec(memory_space=pl.ANY)
    vmem = pl.BlockSpec(memory_space=pltpu.VMEM)
    dma = pltpu.SemaphoreType.DMA
    full, low_rank = pl.pallas_call(
        comm_kernel,
        out_shape=(
            jax.ShapeDtypeStruct((2, 4, 2) + half, BF16),
            jax.ShapeDtypeStruct((4, piece, rank), F32),
        ),
        in_specs=[anyspace] * 5,
        out_specs=(vmem, vmem),
        scratch_shapes=[
            pltpu.VMEM((2 * tok, 16 * rank), BF16),
            pltpu.VMEM((16 * rank, rank), BF16),
            pltpu.VMEM((2, 2 * tok, ff // 4), BF16),
            pltpu.VMEM((2, 2 * tok, rank), F32),
            pltpu.VMEM((rank, 2 * tok), BF16),
            pltpu.VMEM((2, piece, rank), F32),
            pltpu.VMEM((4, 2) + half, BF16),
            pltpu.VMEM((2,) + half, BF16),
            pltpu.VMEM((2, 2) + half, BF16),
            pltpu.VMEM((2,) + half, BF16),
            pltpu.VMEM((2,) + half, BF16),
            pltpu.VMEM((2,) + small, BF16),
            pltpu.VMEM((2, 2) + small, BF16),
            pltpu.VMEM((2,) + small, BF16),
            pltpu.VMEM((2,) + small, BF16),
            pltpu.VMEM((8, piece, rank), BF16),
            pltpu.VMEM((piece, rank), F32),
            dma((6,)), dma((2,)), dma((16,)), dma((16,)), dma((1,)), dma((1,)), dma((2,)), dma((2,)),
            dma((2,)), dma((2,)),
            dma((6,)), dma((6,)), dma((6,)), dma((6,)), dma((4,)), dma((8,)), dma((8,)), dma((4,)),
            dma((8,)), dma((4,)), dma((6,)), dma((6,)), dma((6,)), dma((6,)), dma((8,)), dma((8,)),
        ],
        compiler_params=pltpu.CompilerParams(
            collective_id=0, has_side_effects=True, vmem_limit_bytes=40 << 20
        ),
        name="exchange",
    )(inputs, grad_out, projection, moment, second)
    low_rank = low_rank.reshape(4 * piece, rank)
    state = pl.BlockSpec((4 * piece, rank), lambda i: (0, 0))
    return pl.pallas_call(
        update_kernel,
        grid=(16,),
        out_shape=(
            jax.ShapeDtypeStruct((rank, ff), BF16),
            jax.ShapeDtypeStruct(moment.shape, F32),
            jax.ShapeDtypeStruct(second.shape, F32),
        ),
        in_specs=[
            pl.BlockSpec((2, 4, 2) + half, lambda i: (0,) * 7),
            state,
            pl.BlockSpec((rank, rank), lambda i: (0, 0)),
            state,
            state,
        ],
        out_specs=(pl.BlockSpec((rank, 8 * piece), lambda i: (0, i)), state, state),
        compiler_params=pltpu.CompilerParams(vmem_limit_bytes=20 << 20),
        name="update",
    )(full, low_rank, projection, moment, second)


def solution(mesh):
    split = Mesh(mesh.devices.reshape(2, 8, 2, 4, 2), AXES)
    return jax.shard_map(
        local,
        mesh=split,
        in_specs=(P(AXES, None), P(AXES, None), P(FSDP, None), P(FSDP, None), P(FSDP, None)),
        out_specs=(P(FSDP, None), P(FSDP, None), P(FSDP, None)),
        check_vma=False,
    )
```
